32 devices in a mesh: row: 4 (over x, core), col: 4 (over z), head: 2 (over y).
Axes of the slice: x: 2, y: 2, z: 4, core: 2. Of those that a mesh axis runs over, the one named last changes fastest.
Arguments:
- query_map: bfloat16 [64, 128, 3072], P('row', 'col', 'head'), may hold values from -6 to 6
- key_map: bfloat16 [64, 128, 3072], P('row', 'col', 'head'), may hold values from -7 to 7
- value_map: bfloat16 [64, 128, 3072], P('row', 'col', 'head'), may hold values from -6 to 6
- window_mask: int32 [4, 4, 13, 13], P('row', 'col'), may hold values 0 or 1
- tile_radius: int32 [4, 4], P('row', 'col'), may hold values from 3 to 6, as said below
- dilation_per_tile: int32 [4, 4], P('row', 'col'), may hold values from 1 to 3, as said below
- rel_bias: float32 [48, 13, 13], P('head'), may hold values from -4 to 4
- out_weight: bfloat16 [3072, 3072], P('head'), may hold values from -0.109375 to 0.109375
Outputs:
- mixed: bfloat16 [64, 128, 3072], P('row', 'col', 'head')
The draws below stay inside these ranges and needn't reach their ends.
Inputs may be any that keep to these rules, and one draw needn't show every extreme that they name: `tile_radius`: in each row of tiles, at least one tile has radius 6 and dilation 3. `dilation_per_tile`: in each row of tiles, at least one tile has radius 6 and dilation 3.
All inputs are finite; a program needn't handle non-finite values. No bound on the sum of `window_mask` on one device may be relied on, other than what follows from the above.
Results may differ from the reference program's by a relative error of at most 0.0073.
Values may be sent and summed in bfloat16 or wider, within the bound.
A program may use at most 384 MiB of HBM per device.

```python
import math
from functools import partial
import jax
import jax.numpy as jnp
from jax import lax

TILE_ROWS = 16
TILE_COLS = 32
HEADS = 48
HEAD_DIM = 64
RADIUS_MAX = 6
DILATION_LIMIT = 3
WINDOW = 13
HALO = 18
FEATURES = 3072
MODEL = 3072
ROWS = 64
COLS = 128
N_ROW = 4
N_COL = 4


def draw_query_map(key, part):
    drawn = jax.random.normal(jax.random.fold_in(key, 3), (ROWS, COLS, FEATURES), jnp.float32)
    return jnp.clip(drawn, -6.0, 6.0).astype(jnp.bfloat16)


def draw_key_map(key, part):
    drawn = jax.random.normal(jax.random.fold_in(key, 5), (ROWS, COLS, FEATURES), jnp.float32)
    return jnp.clip(drawn, -6.0, 6.0).astype(jnp.bfloat16)


def window_settings(key):
    base = jax.random.fold_in(key, 29)
    pick_key, radius_key, dilation_key = jax.random.split(base, 3)
    chosen_col = jax.random.randint(pick_key, (N_ROW,), 0, N_COL)
    radius = jax.random.randint(radius_key, (N_ROW, N_COL), 3, RADIUS_MAX + 1)
    dilation = jax.random.randint(dilation_key, (N_ROW, N_COL), 1, DILATION_LIMIT + 1)
    widest = jnp.arange(N_COL, dtype=jnp.int32)[None, :] == chosen_col[:, None]
    radius = jnp.where(widest, RADIUS_MAX, radius).astype(jnp.int32)
    dilation = jnp.where(widest, DILATION_LIMIT, dilation).astype(jnp.int32)
    return (radius, dilation)


def draw_tile_radius(key, part):
    return window_settings(key)[0]


def draw_dilation_per_tile(key, part):
    return window_settings(key)[1]


def touch_ends(result, own_key, smallest, top_value):
    index_at = [jax.random.randint(jax.random.fold_in(own_key, axis), (), 0, length) for axis, length in enumerate(result.shape)]
    longest = result.shape.index(max(result.shape))
    next_to = index_at[:longest] + [(index_at[longest] + 1) % result.shape[longest]] + index_at[longest + 1:]
    return result.at[tuple(index_at)].set(smallest).at[tuple(next_to)].set(top_value)


def shard_levels(key, shape, cuts, low, high):
    gain, own = 1.0, jax.random.fold_in(key, 6)
    for position, parts in cuts:
        draws = jnp.exp(jax.random.uniform(jax.random.fold_in(own, position), (parts,), jnp.float32, low / len(cuts), high / len(cuts)))
        gain = gain * jnp.repeat(draws, shape[position] // parts).reshape([-1 if axis == position else 1 for axis in range(len(shape))])
    return gain


def gaussian(rng, dims, width, limit, pieces=(), kind=jnp.bfloat16):
    values = width * jax.random.normal(rng, dims, jnp.float32)
    if pieces:
        values = values * shard_levels(rng, dims, pieces, -0.22, 0.18)
    return jnp.clip(values, -limit, limit).astype(kind)


def setup_inputs(seed: int = 0) -> dict:
    keys = jax.random.split(jax.random.key(seed), 9)
    query_map = draw_query_map(jax.random.fold_in(keys[8], 71), 0)
    key_map = draw_key_map(jax.random.fold_in(keys[8], 71), 0)
    value_map = gaussian(keys[2], (ROWS, COLS, FEATURES), 1.0, 6.0, ((0, 4), (1, 4), (2, 2)))
    window_mask = touch_ends((jax.random.randint(keys[3], (N_ROW, N_COL, WINDOW, WINDOW), 0, 4) < 3).astype(jnp.int32), jax.random.fold_in(keys[3], 1), 0, 1)
    tile_radius = draw_tile_radius(jax.random.fold_in(keys[8], 71), 0)
    dilation_per_tile = draw_dilation_per_tile(jax.random.fold_in(keys[8], 71), 0)
    rel_bias = gaussian(keys[6], (HEADS, WINDOW, WINDOW), 1.0, 4.0, ((0, 2),), jnp.float32)
    out_weight = gaussian(keys[7], (FEATURES, MODEL), FEATURES ** -0.5, 0.109375, ((0, 2),))
    return {"query_map": query_map, "key_map": key_map, "value_map": value_map, "window_mask": window_mask, "tile_radius": tile_radius, "dilation_per_tile": dilation_per_tile, "rel_bias": rel_bias, "out_weight": out_weight}


def tile_attention(index, query_map, padded_keys, padded_values, window_mask, tile_radius, dilation_per_tile, rel_bias):
    tile_row = index // N_COL
    tile_col = index % N_COL
    row_anchor = tile_row * TILE_ROWS
    col_anchor = tile_col * TILE_COLS
    zero_index = jnp.int32(0)
    queries = lax.dynamic_slice(query_map, (row_anchor, col_anchor, zero_index), (TILE_ROWS, TILE_COLS, FEATURES))
    queries = queries.astype(jnp.float32).reshape(TILE_ROWS, TILE_COLS, HEADS, HEAD_DIM)
    key_block = lax.dynamic_slice(padded_keys, (row_anchor, col_anchor, zero_index), (TILE_ROWS + 2 * HALO, TILE_COLS + 2 * HALO, FEATURES))
    value_block = lax.dynamic_slice(padded_values, (row_anchor, col_anchor, zero_index), (TILE_ROWS + 2 * HALO, TILE_COLS + 2 * HALO, FEATURES))
    radius = tile_radius[tile_row, tile_col]
    dilation = dilation_per_tile[tile_row, tile_col]
    pattern = window_mask[tile_row, tile_col]
    rows_here = row_anchor + jnp.arange(TILE_ROWS, dtype=jnp.int32)
    cols_here = col_anchor + jnp.arange(TILE_COLS, dtype=jnp.int32)
    score_scale = 1.0 / math.sqrt(HEAD_DIM)
    score_list = []
    mask_list = []
    starts = []
    for row_step in range(-RADIUS_MAX, RADIUS_MAX + 1):
        for col_step in range(-RADIUS_MAX, RADIUS_MAX + 1):
            row_start = HALO + row_step * dilation
            col_start = HALO + col_step * dilation
            starts.append((row_start, col_start))
            shifted = lax.dynamic_slice(key_block, (row_start, col_start, zero_index), (TILE_ROWS, TILE_COLS, FEATURES))
            shifted = shifted.astype(jnp.float32).reshape(TILE_ROWS, TILE_COLS, HEADS, HEAD_DIM)
            score = lax.optimization_barrier(jnp.sum(queries * shifted, axis=-1)) * score_scale
            score = score + rel_bias[:, row_step + RADIUS_MAX, col_step + RADIUS_MAX][None, None, :]
            inside = pattern[row_step + RADIUS_MAX, col_step + RADIUS_MAX] == 1
            if row_step == 0 and col_step == 0:
                inside = jnp.logical_or(inside, True)
            inside = inside & (abs(row_step) <= radius) & (abs(col_step) <= radius)
            row_global = rows_here + row_step * dilation
            col_global = cols_here + col_step * dilation
            row_fine = (row_global >= 0) & (row_global < ROWS)
            column_offset = (col_global >= 0) & (col_global < COLS)
            mask_list.append(inside & row_fine[:, None] & column_offset[None, :])
            score_list.append(score)
    scores = jnp.stack(score_list)
    masks = jnp.stack(mask_list)[..., None]
    peak_score = lax.optimization_barrier(jnp.max(jnp.where(masks, scores, -1e+30), axis=0, keepdims=True))
    exponent = jnp.where(masks, jnp.exp(jnp.where(masks, scores - peak_score, -60.0)), 0.0)
    denominator = lax.optimization_barrier(jnp.sum(exponent, axis=0, keepdims=True))
    weights = (exponent / denominator).astype(jnp.bfloat16)
    attended = jnp.zeros((TILE_ROWS, TILE_COLS, HEADS, HEAD_DIM), jnp.float32)
    for place in range(len(starts)):
        row_start, col_start = starts[place]
        shifted = lax.dynamic_slice(value_block, (row_start, col_start, zero_index), (TILE_ROWS, TILE_COLS, FEATURES))
        shifted = shifted.astype(jnp.float32).reshape(TILE_ROWS, TILE_COLS, HEADS, HEAD_DIM)
        attended = attended + weights[place].astype(jnp.float32)[..., None] * shifted
    return attended.reshape(TILE_ROWS, TILE_COLS, FEATURES).astype(jnp.bfloat16)

def reference(query_map, key_map, value_map, window_mask, tile_radius, dilation_per_tile, rel_bias, out_weight):
    padding = ((HALO, HALO), (HALO, HALO), (0, 0))
    padded_keys = jnp.pad(key_map, padding)
    padded_values = jnp.pad(value_map, padding)
    worker = partial(tile_attention, query_map=query_map, padded_keys=padded_keys, padded_values=padded_values, window_mask=window_mask, tile_radius=tile_radius, dilation_per_tile=dilation_per_tile, rel_bias=rel_bias)
    tiles = lax.map(worker, jnp.arange(N_ROW * N_COL, dtype=jnp.int32))
    tiles = tiles.reshape(N_ROW, N_COL, TILE_ROWS, TILE_COLS, FEATURES).transpose(0, 2, 1, 3, 4)
    attended = tiles.reshape(ROWS * COLS, FEATURES)
    mixed = jnp.dot(attended, out_weight, preferred_element_type=jnp.float32).astype(jnp.bfloat16)
    return mixed.reshape(ROWS, COLS, MODEL)
```

```python
import functools
import math

import jax
import jax.numpy as jnp
from jax import lax
from jax.experimental import pallas as pl
from jax.experimental.pallas import tpu as pltpu
from jax.sharding import PartitionSpec as P

HEAD_DIM = 64
RADIUS_MAX = 6
WINDOW = 13
HALO = 18
GROUP = 4
GROUP_FEATURES = GROUP * HEAD_DIM
MASKED = -1e30


def shifted(value, axis, steps):
    count = lax.axis_size(axis)
    first, last = (max(0, -steps), min(count, count - steps))
    return lax.ppermute(value, axis, [(source, source + steps) for source in range(first, last)])


def widen_cols(block, key_cols):
    width = block.shape[2]
    left = shifted(block[:, :, width - HALO :], "col", 1)
    right = shifted(block[:, :, :HALO], "col", -1)
    return left, right


def widen_rows(block):
    height = block.shape[1]
    spill = HALO - height
    above = shifted(block, "row", 1)
    below = shifted(block, "row", -1)
    far_above = shifted(above[:, height - spill :], "row", 1)
    far_below = shifted(below[:, :spill], "row", -1)
    return jnp.concatenate([far_above, above, block, below, far_below], axis=1)


def attention_kernel(rows, dilation_ref, q_ref, k_ref, v_ref, bias_ref, row_ref, out_ref):
    dilation = dilation_ref[0]
    cols = q_ref.shape[1]
    lane_head = lax.broadcasted_iota(jnp.int32, (cols, GROUP_FEATURES), 1) // HEAD_DIM

    def one_row(i, carry):
        query = q_ref[i] * jnp.bfloat16(1.0 / math.sqrt(HEAD_DIM))
        zero = jnp.zeros_like(query)
        stacked = jnp.concatenate(
            [jnp.where(lane_head == h, query, zero) for h in range(GROUP)], axis=0
        )
        places = [i + HALO + (a - RADIUS_MAX) * dilation for a in range(WINDOW)]
        keys = jnp.concatenate([k_ref[place] for place in places], axis=0)
        scores = lax.dot_general(
            stacked, keys, (((1,), (1,)), ((), ())), preferred_element_type=jnp.float32
        )
        scores = scores + bias_ref[0] + row_ref[pl.ds(i, 1), :]
        peak = jnp.max(scores, axis=1, keepdims=True)
        exponent = jnp.exp(scores - peak)
        total = jnp.sum(exponent, axis=1, keepdims=True)
        values = jnp.concatenate([v_ref[place] for place in places], axis=0)
        summed = jnp.dot(
            exponent.astype(jnp.bfloat16), values, preferred_element_type=jnp.float32
        )
        summed = summed / total
        result = summed[:cols]
        for h in range(1, GROUP):
            result = jnp.where(lane_head == h, summed[h * cols : (h + 1) * cols], result)
        out_ref[i] = result.astype(jnp.bfloat16)
        return carry

    lax.fori_loop(0, rows, one_row, 0)


def attend(dilation, query, keys, values, bias, row_bias, first_group):
    rows, cols, features = query.shape
    groups = features // GROUP_FEATURES
    span_rows, span_cols = keys.shape[:2]
    stacked, depth = bias.shape[1:]
    return pl.pallas_call(
        functools.partial(attention_kernel, rows),
        grid=(groups,),
        in_specs=[
            pl.BlockSpec(memory_space=pltpu.SMEM),
            pl.BlockSpec((rows, cols, GROUP_FEATURES), lambda g: (0, 0, g)),
            pl.BlockSpec((span_rows, span_cols, GROUP_FEATURES), lambda g: (0, 0, g)),
            pl.BlockSpec((span_rows, span_cols, GROUP_FEATURES), lambda g: (0, 0, g)),
            pl.BlockSpec((1, stacked, depth), lambda g: (g + first_group, 0, 0)),
            pl.BlockSpec((rows, depth), lambda g: (0, 0)),
        ],
        out_specs=pl.BlockSpec((rows, cols, GROUP_FEATURES), lambda g: (0, 0, g)),
        out_shape=jax.ShapeDtypeStruct((rows, cols, features), jnp.bfloat16),
        compiler_params=pltpu.CompilerParams(vmem_limit_bytes=40 * 1024 * 1024),
        cost_estimate=pl.CostEstimate(
            flops=groups * rows * 16 * stacked * depth * GROUP_FEATURES,
            bytes_accessed=keys.size * 4,
            transcendentals=groups * rows * stacked * depth,
        ),
    )(dilation, query, keys, values, bias, row_bias)


def bias_tables(rel_bias, pattern, radius, dilation, tile_rows, tile_cols, key_cols):
    heads = rel_bias.shape[0]
    groups = heads // GROUP
    total_rows = tile_rows * lax.axis_size("row")
    total_cols = tile_cols * lax.axis_size("col")
    row_anchor = lax.axis_index("row") * tile_rows
    col_anchor = lax.axis_index("col") * tile_cols
    steps = jnp.arange(WINDOW, dtype=jnp.int32) - RADIUS_MAX
    spot = jnp.arange(key_cols, dtype=jnp.int32)
    offset = jnp.where(
        spot < tile_cols, spot, jnp.where(spot < tile_cols + HALO, spot - tile_cols - HALO, spot - HALO)
    )
    real = spot < tile_cols + 2 * HALO
    column = jnp.arange(tile_cols, dtype=jnp.int32)
    gap = offset[None, :] - column[:, None]
    global_col = col_anchor + offset
    inside = (real & (global_col >= 0) & (global_col < total_cols))[None, :]
    chosen = (pattern == 1) | ((steps[:, None] == 0) & (steps[None, :] == 0))
    chosen = chosen & (jnp.abs(steps)[:, None] <= radius) & (jnp.abs(steps)[None, :] <= radius)
    table = jnp.where(chosen[None], rel_bias, MASKED).reshape(groups, GROUP, 1, WINDOW, WINDOW)
    full = jnp.full((groups, GROUP, tile_cols, WINDOW, key_cols), MASKED, jnp.float32)
    for b in range(WINDOW):
        hit = (gap == (b - RADIUS_MAX) * dilation) & inside
        full = jnp.where(hit[None, None, :, None, :], table[..., b][..., None], full)
    full = full.reshape(groups, GROUP * tile_cols, WINDOW * key_cols)
    row_global = row_anchor + jnp.arange(tile_rows)[:, None] + steps[None, :] * dilation
    row_fine = (row_global >= 0) & (row_global < total_rows)
    row_bias = jnp.where(row_fine, 0.0, MASKED).astype(jnp.float32)
    row_bias = jnp.broadcast_to(row_bias[:, :, None], (tile_rows, WINDOW, key_cols))
    return full, row_bias.reshape(tile_rows, WINDOW * key_cols)


def shards(
    query_map, key_map, value_map, window_mask, tile_radius, dilation_per_tile, rel_bias, out_weight
):
    tile_rows, tile_cols, features = query_map.shape
    key_cols = -(-(tile_cols + 2 * HALO) // 16) * 16
    dilation = dilation_per_tile[0, 0]
    bias, row_bias = bias_tables(
        rel_bias, window_mask[0, 0], tile_radius[0, 0], dilation, tile_rows, tile_cols, key_cols
    )
    groups = features // GROUP_FEATURES
    chunks = 3 if groups % 3 == 0 else 1
    width = features // chunks
    pieces = []
    for c in range(chunks):
        cut = slice(c * width, (c + 1) * width)
        pair = jnp.stack([key_map[..., cut], value_map[..., cut]])
        left, right = widen_cols(pair, key_cols)
        fill = jnp.zeros((2, tile_rows, key_cols - tile_cols - 2 * HALO, width), pair.dtype)
        halo = widen_rows(jnp.concatenate([left, right], axis=2))
        own = widen_rows(pair)
        fill = jnp.zeros((2, own.shape[1], key_cols - tile_cols - 2 * HALO, width), pair.dtype)
        wide = jnp.concatenate([own, halo, fill], axis=2)
        pieces.append(
            attend(
                dilation.reshape(1), query_map[..., cut], wide[0], wide[1], bias, row_bias,
                c * (groups // chunks),
            )
        )
    attended = jnp.concatenate(pieces, axis=2).reshape(tile_rows * tile_cols, features)
    count = lax.axis_size("head")
    model = out_weight.shape[1]
    if count != 2:
        partials = jnp.dot(attended, out_weight, preferred_element_type=jnp.float32)
        mixed = lax.psum_scatter(partials, "head", scatter_dimension=1, tiled=True)
        return mixed.astype(jnp.bfloat16).reshape(tile_rows, tile_cols, model // count)
    me = lax.axis_index("head")
    half = model // 2
    theirs = lax.dynamic_slice_in_dim(out_weight, (1 - me) * half, half, 1)
    mine = lax.dynamic_slice_in_dim(out_weight, me * half, half, 1)
    sent = jnp.dot(attended, theirs, preferred_element_type=jnp.float32).astype(jnp.bfloat16)
    got = lax.ppermute(sent, "head", [(0, 1), (1, 0)])
    kept = jnp.dot(attended, mine, preferred_element_type=jnp.float32)
    mixed = (kept + got.astype(jnp.float32)).astype(jnp.bfloat16)
    return mixed.reshape(tile_rows, tile_cols, half)


def solution(mesh):
    placed = (
        P("row", "col", "head"),
        P("row", "col", "head"),
        P("row", "col", "head"),
        P("row", "col", None, None),
        P("row", "col"),
        P("row", "col"),
        P("head", None, None),
        P("head", None),
    )
    return jax.shard_map(
        shards, mesh=mesh, in_specs=placed, out_specs=P("row", "col", "head"), check_vma=False
    )
```

```python
import functools
import math

import jax
import jax.numpy as jnp
from jax import lax
from jax.experimental import pallas as pl
from jax.experimental.pallas import tpu as pltpu
from jax.sharding import PartitionSpec as P

HEAD_DIM = 64
RADIUS_MAX = 6
WINDOW = 13
HALO = 18
GROUP = 4
GROUP_FEATURES = GROUP * HEAD_DIM
MASKED = -1e30


def shifted(value, axis, steps):
    count = lax.axis_size(axis)
    first, last = (max(0, -steps), min(count, count - steps))
    return lax.ppermute(value, axis, [(source, source + steps) for source in range(first, last)])


def attention_kernel(
    rows, first_row, dilation_ref, q_ref, *refs
):
    pieces, (spot_ref, table_ref, row_ref, out_ref, kv_ref, bias_ref) = refs[:5], refs[5:]
    dilation = dilation_ref[0]
    cols = q_ref.shape[1]
    lane_head = lax.broadcasted_iota(jnp.int32, (cols, GROUP_FEATURES), 1) // HEAD_DIM

    filled = pieces[0].shape[2]
    tail = filled // 16 * 16
    top = 0
    for piece in pieces:
        count = piece.shape[1]
        for which in range(2):
            kv_ref[which, top : top + count, tail:] = jnp.zeros(
                (count, kv_ref.shape[2] - tail, GROUP_FEATURES), jnp.bfloat16
            )
            kv_ref[which, top : top + count, :filled] = piece[which]
        top += count
    spot = spot_ref[...]
    for h in range(GROUP):
        table = jnp.full(spot.shape, MASKED, jnp.float32)
        for b in range(WINDOW):
            table = jnp.where(spot == b, table_ref[h, b : b + 1, :], table)
        bias_ref[h * cols : (h + 1) * cols] = table

    def one_row(i, carry):
        query = q_ref[i] * jnp.bfloat16(1.0 / math.sqrt(HEAD_DIM))
        zero = jnp.zeros_like(query)
        stacked = jnp.concatenate(
            [jnp.where(lane_head == h, query, zero) for h in range(GROUP)], axis=0
        )
        places = [i + first_row + HALO + (a - RADIUS_MAX) * dilation for a in range(WINDOW)]
        keys = jnp.concatenate([kv_ref[0, place] for place in places], axis=0)
        scores = lax.dot_general(
            stacked, keys, (((1,), (1,)), ((), ())), preferred_element_type=jnp.float32
        )
        scores = scores + bias_ref[...] + row_ref[pl.ds(i, 1), :]
        peak = jnp.max(scores, axis=1, keepdims=True)
        exponent = jnp.exp(scores - peak)
        total = jnp.sum(exponent, axis=1, keepdims=True)
        values = jnp.concatenate([kv_ref[1, place] for place in places], axis=0)
        summed = jnp.dot(
            exponent.astype(jnp.bfloat16), values, preferred_element_type=jnp.float32
        )
        summed = summed / total
        result = summed[:cols]
        for h in range(1, GROUP):
            result = jnp.where(lane_head == h, summed[h * cols : (h + 1) * cols], result)
        out_ref[i] = result.astype(jnp.bfloat16)
        return carry

    lax.fori_loop(0, rows, one_row, 0)


def attend(dilation, query, pieces, spot, table, row_bias, first_group, groups, part, parts):
    tile_rows, cols, _ = query.shape
    rows = tile_rows // parts
    depth = spot.shape[1]
    key_cols = depth // WINDOW
    span_rows = sum(piece.shape[1] for piece in pieces)
    stacked = GROUP * cols
    return pl.pallas_call(
        functools.partial(attention_kernel, rows, part * rows),
        grid=(groups,),
        in_specs=[
            pl.BlockSpec(memory_space=pltpu.SMEM),
            pl.BlockSpec((rows, cols, GROUP_FEATURES), lambda g: (part, 0, g + first_group)),
            *[
                pl.BlockSpec((*piece.shape[:3], GROUP_FEATURES), lambda g: (0, 0, 0, g))
                for piece in pieces
            ],
            pl.BlockSpec((cols, depth), lambda g: (0, 0)),
            pl.BlockSpec((GROUP, WINDOW, depth), lambda g: (g + first_group, 0, 0)),
            pl.BlockSpec((rows, depth), lambda g: (part, 0)),
        ],
        out_specs=pl.BlockSpec((rows, cols, GROUP_FEATURES), lambda g: (0, 0, g)),
        out_shape=jax.ShapeDtypeStruct((rows, cols, groups * GROUP_FEATURES), jnp.bfloat16),
        scratch_shapes=[
            pltpu.VMEM((2, span_rows, key_cols, GROUP_FEATURES), jnp.bfloat16),
            pltpu.VMEM((stacked, depth), jnp.float32),
        ],
        compiler_params=pltpu.CompilerParams(vmem_limit_bytes=40 * 1024 * 1024),
        cost_estimate=pl.CostEstimate(
            flops=groups * rows * 12 * stacked * depth * GROUP_FEATURES,
            bytes_accessed=sum(piece.size for piece in pieces) * 2,
            transcendentals=groups * rows * stacked * depth,
        ),
    )(dilation, query, *pieces, spot, table, row_bias)


def bias_parts(rel_bias, pattern, radius, dilation, tile_rows, tile_cols, key_cols):
    heads = rel_bias.shape[0]
    depth = WINDOW * key_cols
    total_rows = tile_rows * lax.axis_size("row")
    total_cols = tile_cols * lax.axis_size("col")
    row_anchor = lax.axis_index("row") * tile_rows
    col_anchor = lax.axis_index("col") * tile_cols
    steps = jnp.arange(WINDOW, dtype=jnp.int32) - RADIUS_MAX
    spot = lax.broadcasted_iota(jnp.int32, (tile_cols, depth), 1) % key_cols
    column = lax.broadcasted_iota(jnp.int32, (tile_cols, depth), 0)
    offset = jnp.where(
        spot < tile_cols, spot, jnp.where(spot < tile_cols + HALO, spot - tile_cols - HALO, spot - HALO)
    )
    real = spot < tile_cols + 2 * HALO
    global_col = col_anchor + offset
    inside = real & (global_col >= 0) & (global_col < total_cols)
    step_of = jnp.full((tile_cols, depth), -1, jnp.int32)
    for b in range(WINDOW):
        hit = (offset - column == (b - RADIUS_MAX) * dilation) & inside
        step_of = jnp.where(hit, b, step_of)
    chosen = (pattern == 1) | ((steps[:, None] == 0) & (steps[None, :] == 0))
    chosen = chosen & (jnp.abs(steps)[:, None] <= radius) & (jnp.abs(steps)[None, :] <= radius)
    table = jnp.where(chosen[None], rel_bias, MASKED).transpose(0, 2, 1)
    table = jnp.broadcast_to(table[..., None], (heads, WINDOW, WINDOW, key_cols))
    row_step = lax.broadcasted_iota(jnp.int32, (tile_rows, depth), 1) // key_cols - RADIUS_MAX
    row_global = (
        row_anchor + lax.broadcasted_iota(jnp.int32, (tile_rows, depth), 0) + row_step * dilation
    )
    row_fine = (row_global >= 0) & (row_global < total_rows)
    row_bias = jnp.where(row_fine, 0.0, MASKED).astype(jnp.float32)
    return step_of, table.reshape(heads, WINDOW, depth), row_bias


def shards(
    query_map, key_map, value_map, window_mask, tile_radius, dilation_per_tile, rel_bias, out_weight
):
    tile_rows, tile_cols, features = query_map.shape
    key_cols = -(-(tile_cols + 2 * HALO) // 16) * 16
    dilation = dilation_per_tile[0, 0]
    spot, table, row_bias = bias_parts(
        rel_bias, window_mask[0, 0], tile_radius[0, 0], dilation, tile_rows, tile_cols, key_cols
    )
    groups = features // GROUP_FEATURES
    chunks = 2 if groups % 2 == 0 else 1
    spill = HALO - tile_rows
    width = features // chunks
    per_chunk = groups // chunks
    parts = 2 if tile_rows % 16 == 0 else 1
    tokens = tile_rows * tile_cols // parts
    blocks = [[] for _ in range(parts)]
    for c in range(chunks):
        cut = slice(c * width, (c + 1) * width)
        pair = jnp.stack([key_map[..., cut], value_map[..., cut]])
        left = shifted(pair[:, :, tile_cols - HALO :], "col", 1)
        right = shifted(pair[:, :, :HALO], "col", -1)
        wide = jnp.concatenate([pair, left, right], axis=2)
        pieces = [
            shifted(wide[:, tile_rows - spill :], "row", 2),
            shifted(wide, "row", 1),
            wide,
            shifted(wide, "row", -1),
            shifted(wide[:, :spill], "row", -2),
        ]
        split = parts if c == chunks - 1 else 1
        outs = [
            attend(
                dilation.reshape(1), query_map, pieces, spot, table, row_bias,
                c * per_chunk, per_chunk, part, split,
            ).reshape(-1, width)
            for part in range(split)
        ]
        for part in range(parts):
            if split == parts:
                blocks[part].append(outs[part])
            else:
                blocks[part].append(outs[0][part * tokens : (part + 1) * tokens])
    attended = [jnp.concatenate(block, axis=1) for block in blocks]
    count = lax.axis_size("head")
    model = out_weight.shape[1]
    if count != 2:
        partials = jnp.dot(
            jnp.concatenate(attended), out_weight, preferred_element_type=jnp.float32
        )
        mixed = lax.psum_scatter(partials, "head", scatter_dimension=1, tiled=True)
        return mixed.astype(jnp.bfloat16).reshape(tile_rows, tile_cols, model // count)
    me = lax.axis_index("head")
    half = model // 2
    theirs = lax.dynamic_slice_in_dim(out_weight, (1 - me) * half, half, 1)
    mine = lax.dynamic_slice_in_dim(out_weight, me * half, half, 1)
    mixed = []
    for block in attended:
        sent = jnp.dot(block, theirs, preferred_element_type=jnp.float32).astype(jnp.bfloat16)
        got = lax.ppermute(sent, "head", [(0, 1), (1, 0)])
        kept = jnp.dot(block, mine, preferred_element_type=jnp.float32)
        mixed.append((kept + got.astype(jnp.float32)).astype(jnp.bfloat16))
    return jnp.concatenate(mixed).reshape(tile_rows, tile_cols, half)


def solution(mesh):
    placed = (
        P("row", "col", "head"),
        P("row", "col", "head"),
        P("row", "col", "head"),
        P("row", "col", None, None),
        P("row", "col"),
        P("row", "col"),
        P("head", None, None),
        P("head", None),
    )
    return jax.shard_map(
        shards, mesh=mesh, in_specs=placed, out_specs=P("row", "col", "head"), check_vma=False
    )
```
